512 devices in a mesh: seq: 64 (over z, x, core), chan: 8 (over y).
Axes of the slice: x: 4, y: 8, z: 8, core: 2. Of those that a mesh axis runs over, the one named last changes fastest.
Arguments:
- step_size: bfloat16 [2, 5120, 8192], P(None, ('chan', 'seq')), as said below
- inputs: bfloat16 [2, 5120, 8192], P(None, ('chan', 'seq')), may hold values from -6 to 6
- gate_input: bfloat16 [2, 5120, 8192], P(None, ('chan', 'seq')), may hold values from -6 to 6
- decay_rate: float32 [5120], P('chan'), as said below
- norm_gain: float32 [5120], P('chan'), may hold values from 0.1 to 1.9
- resets: int32 [2, 8], replicated, may hold values from 1 to 8191
Outputs:
- normed: bfloat16 [2, 5120, 8192], P(None, 'chan', 'seq')
The draws below stay inside these ranges and needn't reach their ends.
Inputs may be any that keep to these rules, and one draw needn't show every extreme that they name: `step_size`: positive step sizes. `decay_rate`: positive rates. `resets`: positions within the sequence; several may coincide.
All inputs are finite; a program needn't handle non-finite values.
Results may differ from the reference program's by a relative error of at most 0.001.
Values may be sent and summed in bfloat16 or wider, within the bound.
No kernel may reach another device: no remote copies, remote signals or barrier semaphores. Data moves between devices by JAX's collectives and lax.ppermute only.
A program may use at most 64 MiB of HBM per device.

```python
import math
import jax
import jax.numpy as jnp
from jax import lax

FEATURE_WIDTH = 5120
BATCH_SIZE = 2
NDOC = 8
TOKENS_PER_ROW = 8192


def draw_step_size(key, part):
    first, second, final_segment = jax.random.split(key, 3)
    starting_index = jnp.exp(jax.random.uniform(first, (BATCH_SIZE, FEATURE_WIDTH, TOKENS_PER_ROW), jnp.float32, math.log(0.5), math.log(2.0)))
    places = jax.random.randint(second, (BATCH_SIZE, 4), 0, TOKENS_PER_ROW)
    restart_flags = jnp.any(places[:, :, None] == jnp.arange(TOKENS_PER_ROW)[None, None, :], axis=1)
    restart_runs = 0.35 * TOKENS_PER_ROW * jax.random.uniform(final_segment, (BATCH_SIZE, FEATURE_WIDTH, TOKENS_PER_ROW), jnp.float32, 0.7, 1.4)
    return jnp.where(restart_flags[:, None, :], restart_runs, starting_index).astype(jnp.bfloat16)


def draw_decay_rate(key, part):
    first, second, final_segment = jax.random.split(key, 3)
    slow = jnp.exp(jax.random.uniform(first, (FEATURE_WIDTH,), jnp.float32, math.log(0.5 / TOKENS_PER_ROW), math.log(2.0 / TOKENS_PER_ROW)))
    quick = jnp.exp(jax.random.uniform(second, (FEATURE_WIDTH,), jnp.float32, math.log(2.0 / TOKENS_PER_ROW), math.log(0.05)))
    share = 0.5
    picks = jax.random.uniform(final_segment, (FEATURE_WIDTH,), jnp.float32) < share
    return jnp.where(picks, slow, quick).astype(jnp.float32)


def touch_ends(drawn, own_key, low, largest):
    shape = drawn.shape
    index_at = [jax.random.randint(jax.random.fold_in(own_key, axis), (), 0, shape[axis]) for axis in range(len(shape))]
    drawn = drawn.at[tuple(index_at)].set(low)
    longest = shape.index(max(shape))
    index_at[longest] = (index_at[longest] + 1) % shape[longest]
    return drawn.at[tuple(index_at)].set(largest)


def steps_of(key, shape, cuts, least, high):
    gain, own = 1.0, jax.random.fold_in(key, 6)
    for axis_at, shards_of in cuts:
        steps = jnp.exp(jax.random.uniform(jax.random.fold_in(own, axis_at), (shards_of,), jnp.float32, least / len(cuts), high / len(cuts)))
        gain = gain * jnp.repeat(steps, shape[axis_at] // shards_of).reshape([-1 if axis == axis_at else 1 for axis in range(len(shape))])
    return gain


def bell_draw(rng, dims, scale, most, cuts=(), held_as=jnp.bfloat16):
    values = scale * jax.random.normal(rng, dims, jnp.float32)
    if cuts:
        values = values * steps_of(rng, dims, cuts, -0.22, 0.18)
    return jnp.clip(values, -most, most).astype(held_as)


def setup_inputs(seed: int = 0) -> dict:
    key_list = jax.random.split(jax.random.key(seed), 7)
    return {
        "step_size": draw_step_size(jax.random.fold_in(key_list[6], 71), 0),
        "inputs": bell_draw(key_list[1], (BATCH_SIZE, FEATURE_WIDTH, TOKENS_PER_ROW), 1.0, 6.0, ((1, 512),)),
        "gate_input": bell_draw(key_list[2], (BATCH_SIZE, FEATURE_WIDTH, TOKENS_PER_ROW), 1.0, 6.0, ((1, 512),)),
        "decay_rate": draw_decay_rate(jax.random.fold_in(key_list[6], 71), 0),
        "norm_gain": jnp.clip(1.0 + 0.18 * jax.random.normal(key_list[4], (FEATURE_WIDTH,), jnp.float32), 0.1, 1.9),
        "resets": touch_ends(jax.random.randint(key_list[5], (BATCH_SIZE, NDOC), 1, TOKENS_PER_ROW), jax.random.fold_in(key_list[5], 1), 1, TOKENS_PER_ROW - 1).astype(jnp.int32),
    }


def reference(step_size, inputs, gate_input, decay_rate, norm_gain, resets):
    length = step_size.shape[2]
    places = jnp.arange(length, dtype=jnp.int32)
    reset_mask = jnp.any(resets[:, :, None] == places[None, None, :], axis=1)

    def advance(state, pieces):
        steps, values, marks = pieces
        scaled = steps.astype(jnp.float32) * decay_rate[None, :]
        decay = jnp.where(marks[:, None], jnp.float32(0.0), jnp.exp(-scaled))
        drive = jnp.sqrt(-jnp.expm1(-2.0 * scaled)) * values.astype(jnp.float32)
        state = decay * state + drive
        return (state, state)
    start = jnp.zeros((step_size.shape[0], step_size.shape[1]), jnp.float32)
    _, states = lax.scan(advance, start, (jnp.moveaxis(step_size, 2, 0), jnp.moveaxis(inputs, 2, 0), reset_mask.T))
    state = jnp.moveaxis(states, 0, 2)
    gated = state * jax.nn.silu(gate_input.astype(jnp.float32))
    mean_square = lax.optimization_barrier(jnp.mean(gated * gated, axis=1, keepdims=True))
    return (gated * lax.rsqrt(mean_square + 1e-05) * norm_gain[None, :, None]).astype(jnp.bfloat16)
```

```python
import functools
import math

import jax
import jax.numpy as jnp
from jax import lax
from jax.experimental import pallas as pl
from jax.experimental.pallas import tpu as pltpu
from jax.sharding import Mesh
from jax.sharding import PartitionSpec as P

FEATURE_WIDTH = 5120
SEQ = ("seq_0", "seq_1", "seq_2")
CHAN_SEQ = ("chan", "seq_0", "seq_1", "seq_2")
LANES = 128
SUB = 8
LEVELS = 32700.0
MIDDLE = 32768.0
FINE = 64.0
CODE_ZERO = 16384.0
LOG2E = 1.4426950408889634


def one_minus_exp(x, expo):
    t = jnp.minimum(x, 0.5)
    p = jnp.float32(-1.0 / 5040.0)
    p = p * t + jnp.float32(1.0 / 720.0)
    p = 1.0 / 120.0 - p * t
    p = 1.0 / 24.0 - p * t
    p = 1.0 / 6.0 - p * t
    p = 0.5 - p * t
    p = 1.0 - p * t
    return jnp.where(x < 0.5, t * p, 1.0 - expo * expo)


def rolled(x, k):
    return pltpu.roll(x, k, 1)


def scan_kernel(sizes, rate_ref, reset_ref, step_ref, inp_ref, gate_ref, out_ref, xs, marks, tot):
    batch, width, blocks, pitch, ndoc = sizes
    place = lax.axis_index(SEQ)
    groups = blocks // SUB
    rows = batch * width
    lane = lax.broadcasted_iota(jnp.int32, (SUB, LANES), 1)
    sub = lax.broadcasted_iota(jnp.int32, (SUB, LANES), 0)

    def bring(j, _):
        for k, ref in enumerate((step_ref, inp_ref, gate_ref)):
            for b in range(batch):
                for low in range(0, width, SUB):
                    n = min(SUB, width - low)
                    v = ref[b, low : low + n, pl.ds(pl.multiple_of(j * LANES, LANES), LANES)]
                    xs[k, pl.ds((b * width + low) * pitch + j, n, stride=pitch), :] = v.astype(
                        jnp.float32
                    )
        return 0

    lax.fori_loop(0, blocks, bring, 0, unroll=4)

    rate = [rate_ref[place * width + c] for c in range(width)]

    def local(m, _):
        first = m * SUB
        t = (first + sub) * LANES + lane
        ta = jnp.ones((SUB, LANES), jnp.float32)
        tb = jnp.zeros((SUB, LANES), jnp.float32)
        for b in range(batch):
            hit = t == reset_ref[b, 0]
            for k in range(1, ndoc):
                hit = hit | (t == reset_ref[b, k])
            for c in range(width):
                r = b * width + c
                at = pl.ds(r * pitch + first, SUB)
                scaled = xs[0, at, :] * rate[c]
                expo = jnp.exp2(scaled * (-LOG2E))
                drive = jnp.sqrt(one_minus_exp(scaled + scaled, expo)) * xs[1, at, :]
                a = jnp.where(hit, 0.0, expo)
                s = drive
                k = 1
                while k < LANES:
                    keep = lane >= k
                    s = s + a * jnp.where(keep, rolled(s, k), 0.0)
                    a = a * jnp.where(keep, rolled(a, k), 1.0)
                    k *= 2
                xs[0, at, :] = a
                xs[1, at, :] = s
                ta = jnp.where(lane == r, a[:, LANES - 1 :], ta)
                tb = jnp.where(lane == r, s[:, LANES - 1 :], tb)
        here = pl.ds(pl.multiple_of(first, SUB), SUB)
        tot[0, here, :] = ta
        tot[1, here, :] = tb
        return 0

    lax.fori_loop(0, groups, local, 0, unroll=2)

    carry = jnp.zeros((SUB, LANES), jnp.float32)
    for m in range(groups):
        ta = tot[0, m * SUB : (m + 1) * SUB, :]
        tb = tot[1, m * SUB : (m + 1) * SUB, :]
        for k in (1, 2, 4):
            keep = sub >= k
            tb = tb + ta * jnp.where(keep, pltpu.roll(tb, k, 0), 0.0)
            ta = ta * jnp.where(keep, pltpu.roll(ta, k, 0), 1.0)
        full = tb + ta * carry
        tot[0, m * SUB : (m + 1) * SUB, :] = jnp.where(sub == 0, carry, pltpu.roll(full, 1, 0))
        carry = jnp.broadcast_to(full[SUB - 1 :, :], (SUB, LANES))

    def emit(m, _):
        first = m * SUB
        start = tot[0, pl.ds(pl.multiple_of(first, SUB), SUB), :]
        packed = []
        code = None
        for b in range(batch):
            values = []
            top = jnp.full((SUB, LANES), 1e-37, jnp.float32)
            for c in range(width):
                r = b * width + c
                at = pl.ds(r * pitch + first, SUB)
                state = xs[1, at, :] + xs[0, at, :] * start[:, r : r + 1]
                g = xs[2, at, :]
                value = state * (g / (1.0 + jnp.exp2(g * (-LOG2E))))
                values.append(value)
                top = jnp.maximum(top, jnp.abs(value))
            e = jnp.ceil(jnp.log2(top) * FINE)
            inv = jnp.exp2(e * (-1.0 / FINE)) * LEVELS
            whole = [(v * inv + (MIDDLE + 0.5)).astype(jnp.int32) for v in values]
            whole.append((e + CODE_ZERO).astype(jnp.int32))
            packed.append(whole)
        for c in range(width + 1):
            word = packed[0][c] * 65536 | packed[1][c]
            out_ref[pl.ds(first * (width + 1) + c, SUB, stride=width + 1), :] = word
        return 0

    lax.fori_loop(0, groups, emit, 0)


def opened(word):
    return (
        lax.shift_right_logical(word, 16).astype(jnp.float32),
        (word & 65535).astype(jnp.float32),
    )


def scales(word):
    return [jnp.exp2((e - CODE_ZERO) * (1.0 / FINE)) * (1.0 / LEVELS) for e in opened(word)]


def squares_kernel(sizes, got_ref, sum_ref, keep_ref, send_ref):
    width, chips, cores, chan = sizes
    mine = lax.axis_index("seq_2")
    record = width + 1
    acc = [[None, None], [None, None]]
    for m in range(chips // SUB):
        base = m * SUB * cores * record
        codes = [
            got_ref[pl.ds(base + k * record + width, SUB, stride=cores * record), :]
            for k in range(cores)
        ]
        scale = [scales(w) for w in codes]
        for c in range(record):
            words = [
                got_ref[pl.ds(base + k * record + c, SUB, stride=cores * record), :]
                for k in range(cores)
            ]
            to = pl.ds(m * SUB * record + c, SUB, stride=record)
            keep_ref[to, :] = jnp.where(mine == 0, words[0], words[1])
            send_ref[to, :] = jnp.where(mine == 0, words[1], words[0])
            if c < width:
                for k in range(cores):
                    for b, q in enumerate(opened(words[k])):
                        v = (q - MIDDLE) * scale[k][b]
                        acc[k][b] = v * v if acc[k][b] is None else acc[k][b] + v * v
    for k in range(cores):
        for b in range(2):
            row = jnp.sum(acc[k][b], axis=0, keepdims=True)
            for y in range(chan):
                sum_ref[k * chan + y, b : b + 1, :] = row


def final_kernel(sizes, keep_ref, got_ref, sum_ref, gain_ref, out_ref, flat):
    width, chips, cores, peers = sizes
    mine = lax.axis_index("seq_2")
    record = width + 1
    total = sum_ref[0]
    for k in range(1, peers):
        total = total + sum_ref[k]
    norm = lax.rsqrt(total / jnp.float32(FEATURE_WIDTH) + 1e-5)
    for m in range(chips // SUB):
        def words(c):
            at = pl.ds(m * SUB * record + c, SUB, stride=record)
            a, b = keep_ref[at, :], got_ref[at, :]
            return jnp.where(mine == 0, a, b), jnp.where(mine == 0, b, a)

        scale = [scales(w) for w in words(width)]
        scale = [[s * norm[b : b + 1] for b, s in enumerate(pair)] for pair in scale]
        for c in range(width):
            for k, word in enumerate(words(c)):
                for b, q in enumerate(opened(word)):
                    row = m * SUB * cores * width + k * width + c
                    flat[b, pl.ds(row, SUB, stride=cores * width), :] = (q - MIDDLE) * scale[k][b]
    channels = out_ref.shape[1]
    for g in range(channels // LANES):
        gain = jnp.broadcast_to(gain_ref[g : g + 1, :], (LANES, LANES)).T
        for b in range(2):
            rows = slice(g * LANES, (g + 1) * LANES)
            out_ref[b, rows, :] = (flat[b, rows, :] * gain).astype(jnp.bfloat16)


def whole(space=pltpu.VMEM):
    return pl.BlockSpec(memory_space=space)


def per_device(step_size, inputs, gate_input, decay_rate, norm_gain, resets):
    batch, width, length = step_size.shape
    chips = lax.axis_size("seq_0") * lax.axis_size("seq_1")
    cores = lax.axis_size("seq_2")
    chan = lax.axis_size("chan")
    blocks = chips * cores
    record = width + 1
    pitch = blocks
    rows = batch * width
    words = pl.pallas_call(
        functools.partial(scan_kernel, (batch, width, blocks, pitch, resets.shape[1])),
        out_shape=jax.ShapeDtypeStruct((blocks * record, LANES), jnp.int32),
        in_specs=[whole(pltpu.SMEM), whole(pltpu.SMEM), whole(), whole(), whole()],
        out_specs=whole(),
        scratch_shapes=[
            pltpu.VMEM((3, rows * pitch, LANES), jnp.float32),
            pltpu.VMEM((batch, blocks, LANES), jnp.float32),
            pltpu.VMEM((2, blocks, LANES), jnp.float32),
        ],
        name="scan",
    )(decay_rate, resets, step_size, inputs, gate_input)
    words = words.reshape(chips, cores * record, 1, LANES)
    words = lax.all_to_all(words, ("seq_0", "seq_1"), 0, 0, tiled=True)
    words = words.reshape(chips * cores * record, LANES)
    half = jax.ShapeDtypeStruct((chips * record, LANES), jnp.int32)
    sums, keep, send = pl.pallas_call(
        functools.partial(squares_kernel, (width, chips, cores, chan)),
        out_shape=(jax.ShapeDtypeStruct((cores * chan, batch, LANES), jnp.float32), half, half),
        in_specs=[whole()],
        out_specs=(whole(), whole(), whole()),
        name="squares",
    )(words)
    sums = lax.all_to_all(sums, ("seq_2", "chan"), 0, 0, tiled=True)
    got = lax.ppermute(send, "seq_2", [(0, 1), (1, 0)])
    channels = chips * cores * width
    return pl.pallas_call(
        functools.partial(final_kernel, (width, chips, cores, cores * chan)),
        out_shape=jax.ShapeDtypeStruct((batch, channels, LANES), jnp.bfloat16),
        in_specs=[whole()] * 4,
        out_specs=whole(),
        scratch_shapes=[pltpu.VMEM((batch, channels, LANES), jnp.float32)],
        name="final",
    )(keep, got, sums, norm_gain.reshape(channels // LANES, LANES))


def solution(mesh):
    split = Mesh(
        mesh.devices.reshape(8, 4, 2, mesh.shape["chan"]), ("seq_0", "seq_1", "seq_2", "chan")
    )
    in_specs = (
        P(None, CHAN_SEQ, None),
        P(None, CHAN_SEQ, None),
        P(None, CHAN_SEQ, None),
        P("chan"),
        P("chan"),
        P(),
    )
    out_specs = P(None, "chan", SEQ)
    return jax.shard_map(
        per_device, mesh=split, in_specs=in_specs, out_specs=out_specs, check_vma=False
    )
```

```python
import functools
import math

import jax
import jax.numpy as jnp
from jax import lax
from jax.experimental import pallas as pl
from jax.experimental.pallas import tpu as pltpu
from jax.sharding import Mesh
from jax.sharding import PartitionSpec as P

FEATURE_WIDTH = 5120
SEQ = ("seq_0", "seq_1", "seq_2")
CHAN_SEQ = ("chan", "seq_0", "seq_1", "seq_2")
LANES = 128
SUB = 8
LEVELS = 32700.0
MIDDLE = 32768.0
FINE = 64.0
CODE_ZERO = 16384.0
LOG2E = 1.4426950408889634
UNROLL = 2


def root_of_one_minus_exp(x, expo):
    p = 1.0 / 6.0 - x * (1.0 / 24.0 - x * (1.0 / 120.0))
    p = x * (1.0 - x * (0.5 - x * p))
    y = jnp.where(x < 0.0625, p, 1.0 - expo * expo)
    return y * lax.rsqrt(jnp.maximum(y, 1e-37))


def tile(v):
    return slice(v * SUB, (v + 1) * SUB)


def scan_kernel(
    sizes, rate_ref, reset_ref, step_ref, inp_ref, gate_ref, out_ref, part, held, live, top, tot, ints
):
    batch, width, blocks, ndoc = sizes
    place = lax.axis_index(SEQ)
    count = batch * blocks
    tiles = LANES // SUB
    lane = lax.broadcasted_iota(jnp.int32, (SUB, LANES), 1)
    sub = lax.broadcasted_iota(jnp.int32, (SUB, LANES), 0)
    odd = (sub & 1) == 1

    marks = [jnp.where(odd, reset_ref[1, k], reset_ref[0, k]) for k in range(ndoc)]
    for v in range(tiles):
        t = (v * (SUB // 2) + (sub >> 1)) * LANES + lane
        hit = t == marks[0]
        for mark in marks[1:]:
            hit = hit | (t == mark)
        live[tile(v), :] = jnp.where(hit, 0.0, 1.0)
        top[tile(v), :] = jnp.full((SUB, LANES), 1e-37, jnp.float32)
        part[tile(v), :] = jnp.zeros((SUB, LANES), jnp.float32)
    tot[...] = jnp.zeros_like(tot)

    def local(c, _):
        at = pl.ds(pl.multiple_of(c * count, count), count)
        scaled = step_ref[at, :].astype(jnp.float32) * rate_ref[place * width + c]
        expo = jnp.exp2(scaled * (-LOG2E))
        drive = root_of_one_minus_exp(scaled + scaled, expo) * inp_ref[at, :].astype(jnp.float32)
        at_a = (expo * live[...]).T
        at_s = drive.T
        end_a = end_s = None
        for v in range(tiles):
            a, s = at_a[tile(v)], at_s[tile(v)]
            for k in (1, 2, 4):
                keep = sub >= k
                s = s + a * jnp.where(keep, pltpu.roll(s, k, 0), 0.0)
                a = a * jnp.where(keep, pltpu.roll(a, k, 0), 1.0)
            if v:
                s = s + a * end_s
                a = a * end_a
            here = pl.ds(pl.multiple_of(c * count + v * SUB, SUB), SUB)
            held[0, here, :] = a
            held[1, here, :] = s
            end_a = jnp.broadcast_to(a[SUB - 1 :], (SUB, LANES))
            end_s = jnp.broadcast_to(s[SUB - 1 :], (SUB, LANES))
        tot[0, pl.ds(c, 1), :] = end_a[:1]
        tot[1, pl.ds(c, 1), :] = end_s[:1]
        return 0

    lax.fori_loop(0, width, local, 0, unroll=UNROLL)

    wide = lax.broadcasted_iota(jnp.int32, tot.shape[1:], 1)
    a, s = tot[0], tot[1]
    k = batch
    while k < count:
        keep = wide >= k
        s = s + a * jnp.where(keep, pltpu.roll(s, k, 1), 0.0)
        a = a * jnp.where(keep, pltpu.roll(a, k, 1), 1.0)
        k *= 2
    tot[0] = jnp.where(wide >= batch, pltpu.roll(s, batch, 1), 0.0)

    def emit(c, _):
        at = pl.ds(pl.multiple_of(c * count, count), count)
        state = (held[1, at, :] + held[0, at, :] * tot[0, pl.ds(c, 1), :]).T
        g = gate_ref[at, :].astype(jnp.float32)
        value = state * (g / (1.0 + jnp.exp2(g * (-LOG2E))))
        held[2, at, :] = value
        top[...] = jnp.maximum(top[...], jnp.abs(value))
        part[...] = part[...] + value * value
        return 0

    lax.fori_loop(0, width, emit, 0, unroll=UNROLL)

    e = jnp.ceil(jnp.log2(top[...]) * FINE)
    top[...] = jnp.exp2(e * (-1.0 / FINE)) * LEVELS
    ints[pl.ds(width * count, count), :] = (e + CODE_ZERO).astype(jnp.int32)
    for c in range(width):
        ints[tile_of(c, count), :] = (held[2, tile_of(c, count), :] * top[...] + (MIDDLE + 0.5)).astype(
            jnp.int32
        )
    for c in range(width + 1):
        for m in range(blocks // SUB):
            first = ints[pl.ds(c * count + m * SUB * batch, SUB, stride=batch), :]
            second = ints[pl.ds(c * count + m * SUB * batch + 1, SUB, stride=batch), :]
            out_ref[pl.ds(m * SUB * (width + 1) + c, SUB, stride=width + 1), :] = (
                first * 65536 | second
            )


def tile_of(c, count):
    return slice(c * count, (c + 1) * count)


def opened(word):
    return (
        lax.shift_right_logical(word, 16).astype(jnp.float32),
        (word & 65535).astype(jnp.float32),
    )


def scales(word):
    return [jnp.exp2((e - CODE_ZERO) * (1.0 / FINE)) * (1.0 / LEVELS) for e in opened(word)]


def squares_kernel(sizes, got_ref, sum_ref, keep_ref, send_ref):
    width, chips, cores, chan = sizes
    mine = lax.axis_index("seq_2")
    record = width + 1
    acc = [[None, None], [None, None]]
    for m in range(chips // SUB):
        base = m * SUB * cores * record
        codes = [
            got_ref[pl.ds(base + k * record + width, SUB, stride=cores * record), :]
            for k in range(cores)
        ]
        scale = [scales(w) for w in codes]
        for c in range(record):
            words = [
                got_ref[pl.ds(base + k * record + c, SUB, stride=cores * record), :]
                for k in range(cores)
            ]
            to = pl.ds(m * SUB * record + c, SUB, stride=record)
            keep_ref[to, :] = jnp.where(mine == 0, words[0], words[1])
            send_ref[to, :] = jnp.where(mine == 0, words[1], words[0])
            if c < width:
                for k in range(cores):
                    for b, q in enumerate(opened(words[k])):
                        v = (q - MIDDLE) * scale[k][b]
                        acc[k][b] = v * v if acc[k][b] is None else acc[k][b] + v * v
    for k in range(cores):
        for b in range(2):
            row = jnp.sum(acc[k][b], axis=0, keepdims=True)
            for y in range(chan):
                sum_ref[k * chan + y, b : b + 1, :] = row


def final_kernel(sizes, keep_ref, got_ref, sum_ref, gain_ref, out_ref, flat):
    width, chips, cores, peers = sizes
    mine = lax.axis_index("seq_2")
    record = width + 1
    total = sum_ref[0]
    for k in range(1, peers):
        total = total + sum_ref[k]
    norm = lax.rsqrt(total / jnp.float32(FEATURE_WIDTH) + 1e-5)
    for m in range(chips // SUB):
        def words(c):
            at = pl.ds(m * SUB * record + c, SUB, stride=record)
            a, b = keep_ref[at, :], got_ref[at, :]
            return jnp.where(mine == 0, a, b), jnp.where(mine == 0, b, a)

        scale = [scales(w) for w in words(width)]
        scale = [[s * norm[b : b + 1] for b, s in enumerate(pair)] for pair in scale]
        for c in range(width):
            for k, word in enumerate(words(c)):
                for b, q in enumerate(opened(word)):
                    row = m * SUB * cores * width + k * width + c
                    flat[b, pl.ds(row, SUB, stride=cores * width), :] = (q - MIDDLE) * scale[k][b]
    channels = out_ref.shape[1]
    for g in range(channels // LANES):
        gain = jnp.broadcast_to(gain_ref[g : g + 1, :], (LANES, LANES)).T
        for b in range(2):
            rows = slice(g * LANES, (g + 1) * LANES)
            out_ref[b, rows, :] = (flat[b, rows, :] * gain).astype(jnp.bfloat16)


def whole(space=pltpu.VMEM):
    return pl.BlockSpec(memory_space=space)


def room(mebibytes):
    return pltpu.CompilerParams(vmem_limit_bytes=mebibytes * 1024 * 1024)


def per_device(step_size, inputs, gate_input, decay_rate, norm_gain, resets):
    batch, width, length = step_size.shape
    chips = lax.axis_size("seq_0") * lax.axis_size("seq_1")
    cores = lax.axis_size("seq_2")
    chan = lax.axis_size("chan")
    blocks = chips * cores
    record = width + 1
    rows = batch * width * blocks

    def as_rows(array):
        split = array.reshape(batch, width, blocks, LANES)
        return split.transpose(1, 2, 0, 3).reshape(rows, LANES)

    words, part = pl.pallas_call(
        functools.partial(scan_kernel, (batch, width, blocks, resets.shape[1])),
        out_shape=(
            jax.ShapeDtypeStruct((blocks * record, LANES), jnp.int32),
            jax.ShapeDtypeStruct((batch * blocks, LANES), jnp.float32),
        ),
        in_specs=[whole(pltpu.SMEM), whole(pltpu.SMEM), whole(), whole(), whole()],
        out_specs=(whole(), whole()),
        scratch_shapes=[
            pltpu.VMEM((3, rows, LANES), jnp.float32),
            pltpu.VMEM((batch * blocks, LANES), jnp.float32),
            pltpu.VMEM((batch * blocks, LANES), jnp.float32),
            pltpu.VMEM((2, 2 * SUB, LANES), jnp.float32),
            pltpu.VMEM((rows + batch * blocks, LANES), jnp.int32),
        ],
        compiler_params=room(16),
        name="scan",
    )(decay_rate, resets, as_rows(step_size), as_rows(inputs), as_rows(gate_input))
    words = words.reshape(chips, cores * record, 1, LANES)
    words = lax.all_to_all(words, ("seq_0", "seq_1"), 0, 0, tiled=True)
    words = words.reshape(chips * cores * record, LANES)
    half = jax.ShapeDtypeStruct((chips * record, LANES), jnp.int32)
    sums, keep, send = pl.pallas_call(
        functools.partial(squares_kernel, (width, chips, cores, chan)),
        out_shape=(jax.ShapeDtypeStruct((cores * chan, batch, LANES), jnp.float32), half, half),
        in_specs=[whole()],
        out_specs=(whole(), whole(), whole()),
        compiler_params=room(8),
        name="squares",
    )(words)
    sums = lax.all_to_all(sums, ("seq_2", "chan"), 0, 0, tiled=True)
    got = lax.ppermute(send, "seq_2", [(0, 1), (1, 0)])
    channels = chips * cores * width
    return pl.pallas_call(
        functools.partial(final_kernel, (width, chips, cores, cores * chan)),
        out_shape=jax.ShapeDtypeStruct((batch, channels, LANES), jnp.bfloat16),
        in_specs=[whole()] * 4,
        out_specs=whole(),
        scratch_shapes=[pltpu.VMEM((batch, channels, LANES), jnp.float32)],
        compiler_params=room(8),
        name="final",
    )(keep, got, sums, norm_gain.reshape(channels // LANES, LANES))


def solution(mesh):
    split = Mesh(
        mesh.devices.reshape(8, 4, 2, mesh.shape["chan"]), ("seq_0", "seq_1", "seq_2", "chan")
    )
    in_specs = (
        P(None, CHAN_SEQ, None),
        P(None, CHAN_SEQ, None),
        P(None, CHAN_SEQ, None),
        P("chan"),
        P("chan"),
        P(),
    )
    out_specs = P(None, "chan", SEQ)
    return jax.shard_map(
        per_device, mesh=split, in_specs=in_specs, out_specs=out_specs, check_vma=False
    )
```

```python
import functools

import jax
import jax.numpy as jnp
from jax import lax
from jax.experimental import pallas as pl
from jax.experimental.pallas import tpu as pltpu
from jax.sharding import Mesh
from jax.sharding import PartitionSpec as P


FEATURE_WIDTH = 5120
SEQ = ("seq_0", "seq_1", "seq_2")
CHAN_SEQ = ("chan", "seq_0", "seq_1", "seq_2")
LANES = 128
SUB = 8
LEVELS = 32700.0
MIDDLE = 32768.0
FINE = 64.0
CODE_ZERO = 16384.0
CORES = 2
LOG2E = 1.4426950408889634
UNROLL = 2


def root_of_one_minus_exp(x, expo):
    p = 1.0 / 6.0 - x * (1.0 / 24.0 - x * (1.0 / 120.0))
    p = x * (1.0 - x * (0.5 - x * p))
    y = jnp.where(x < 0.0625, p, 1.0 - expo * expo)
    return y * lax.rsqrt(jnp.maximum(y, 1e-37))


def tile(v):
    return slice(v * SUB, (v + 1) * SUB)


def scan_kernel(
    sizes,
    rate_hbm,
    reset_hbm,
    step_hbm,
    inp_hbm,
    gate_hbm,
    out_ref,
    held,
    live,
    top,
    tot,
    ints,
    step_ref,
    inp_ref,
    gate_ref,
    rate_ref,
    reset_ref,
    sems,
    small,
):
    batch, width, blocks, ndoc = sizes
    place = lax.axis_index(SEQ)
    count = batch * blocks
    tiles = LANES // SUB
    lane = lax.broadcasted_iota(jnp.int32, (SUB, LANES), 1)
    sub = lax.broadcasted_iota(jnp.int32, (SUB, LANES), 0)
    odd = (sub & 1) == 1

    sources = ((step_hbm, step_ref), (inp_hbm, inp_ref), (gate_hbm, gate_ref))

    def fetch(k, c):
        at = pl.ds(pl.multiple_of(c * count, count), count)
        return pltpu.make_async_copy(sources[k][0].at[at], sources[k][1].at[at], sems.at[k, c])

    scalars = [
        pltpu.make_async_copy(rate_hbm, rate_ref, small.at[0]),
        pltpu.make_async_copy(reset_hbm, reset_ref, small.at[1]),
    ]
    for copy in scalars:
        copy.start()
    for c in range(width):
        fetch(0, c).start()
        fetch(1, c).start()
    for c in range(width):
        fetch(2, c).start()

    for copy in scalars:
        copy.wait()
    marks = [jnp.where(odd, reset_ref[1, k], reset_ref[0, k]) for k in range(ndoc)]
    for v in range(tiles):
        t = (v * (SUB // 2) + (sub >> 1)) * LANES + lane
        hit = t == marks[0]
        for mark in marks[1:]:
            hit = hit | (t == mark)
        live[tile(v), :] = jnp.where(hit, 0.0, 1.0)
        top[tile(v), :] = jnp.full((SUB, LANES), 1e-37, jnp.float32)
    tot[...] = jnp.zeros_like(tot)

    def local(c, _):
        at = pl.ds(pl.multiple_of(c * count, count), count)
        fetch(0, c).wait()
        fetch(1, c).wait()
        scaled = step_ref[at, :].astype(jnp.float32) * rate_ref[place * width + c]
        expo = jnp.exp2(scaled * (-LOG2E))
        drive = root_of_one_minus_exp(scaled + scaled, expo) * inp_ref[at, :].astype(jnp.float32)
        at_a = (expo * live[...]).T
        at_s = drive.T
        end_a = end_s = None
        for v in range(tiles):
            a, s = at_a[tile(v)], at_s[tile(v)]
            for k in (1, 2, 4):
                keep = sub >= k
                s = s + a * jnp.where(keep, pltpu.roll(s, k, 0), 0.0)
                a = a * jnp.where(keep, pltpu.roll(a, k, 0), 1.0)
            if v:
                s = s + a * end_s
                a = a * end_a
            here = pl.ds(pl.multiple_of(c * count + v * SUB, SUB), SUB)
            held[0, here, :] = a
            held[1, here, :] = s
            end_a = jnp.broadcast_to(a[SUB - 1 :], (SUB, LANES))
            end_s = jnp.broadcast_to(s[SUB - 1 :], (SUB, LANES))
        tot[0, pl.ds(c, 1), :] = end_a[:1]
        tot[1, pl.ds(c, 1), :] = end_s[:1]
        return 0

    lax.fori_loop(0, width, local, 0, unroll=UNROLL)

    wide = lax.broadcasted_iota(jnp.int32, tot.shape[1:], 1)
    a, s = tot[0], tot[1]
    k = batch
    while k < count:
        keep = wide >= k
        s = s + a * jnp.where(keep, pltpu.roll(s, k, 1), 0.0)
        a = a * jnp.where(keep, pltpu.roll(a, k, 1), 1.0)
        k *= 2
    tot[0] = jnp.where(wide >= batch, pltpu.roll(s, batch, 1), 0.0)

    def emit(c, _):
        at = pl.ds(pl.multiple_of(c * count, count), count)
        state = (held[1, at, :] + held[0, at, :] * tot[0, pl.ds(c, 1), :]).T
        fetch(2, c).wait()
        g = gate_ref[at, :].astype(jnp.float32)
        value = state * (g / (1.0 + jnp.exp2(g * (-LOG2E))))
        held[2, at, :] = value
        top[...] = jnp.maximum(top[...], jnp.abs(value))
        return 0

    lax.fori_loop(0, width, emit, 0, unroll=UNROLL)

    e = jnp.ceil(jnp.log2(top[...]) * FINE)
    top[...] = jnp.exp2(e * (-1.0 / FINE)) * LEVELS
    ints[pl.ds(width * count, count), :] = (e + CODE_ZERO).astype(jnp.int32)
    for c in range(width):
        ints[tile_of(c, count), :] = (held[2, tile_of(c, count), :] * top[...] + (MIDDLE + 0.5)).astype(
            jnp.int32
        )
    record = width + 1
    for c in range(record):
        for m in range(blocks // SUB):
            base = c * count + m * SUB * batch
            first, second = [ints[pl.ds(base + b, SUB, stride=batch), :] for b in range(batch)]
            out_ref[pl.ds(m * SUB * record + c, SUB, stride=record), :] = first * 65536 | second


def tile_of(c, count):
    return slice(c * count, (c + 1) * count)


def opened(word):
    return (
        lax.shift_right_logical(word, 16).astype(jnp.float32),
        (word & 65535).astype(jnp.float32),
    )


def scales(word):
    return [jnp.exp2((e - CODE_ZERO) * (1.0 / FINE)) * (1.0 / LEVELS) for e in opened(word)]


def words_at(ref, m, k, c, record):
    return ref[pl.ds((m * SUB * CORES + k) * record + c, SUB, stride=CORES * record), :]


def squares_kernel(sizes, got_ref, sum_ref):
    width, chips = sizes
    record = width + 1
    chan = sum_ref.shape[0] // CORES
    for k in range(CORES):
        acc = [None, None]
        for m in range(chips // SUB):
            scale = scales(words_at(got_ref, m, k, width, record))
            part = [None, None]
            for c in range(width):
                for b, q in enumerate(opened(words_at(got_ref, m, k, c, record))):
                    v = q - MIDDLE
                    part[b] = v * v if part[b] is None else part[b] + v * v
            for b in range(2):
                more = part[b] * (scale[b] * scale[b])
                acc[b] = more if acc[b] is None else acc[b] + more
        for b in range(2):
            row = jnp.sum(acc[b], axis=0, keepdims=True)
            for y in range(chan):
                sum_ref[k * chan + y, b : b + 1, :] = row


def gain_kernel(gain_ref, out_ref):
    for g in range(out_ref.shape[0] // LANES):
        row = gain_ref[g : g + 1, :]
        out_ref[g * LANES : (g + 1) * LANES, :] = jnp.broadcast_to(row, (LANES, LANES)).T


def final_kernel(sizes, own_ref, mate_ref, sum_ref, gain_ref, out_ref, flat):
    width, chips = sizes
    mine = lax.axis_index("seq_2")
    record = width + 1
    total = sum_ref[0]
    for k in range(1, sum_ref.shape[0]):
        total = total + sum_ref[k]
    norm = lax.rsqrt(total / jnp.float32(FEATURE_WIDTH) + 1e-5)
    for m in range(chips // SUB):

        def words(c):
            a = words_at(own_ref, m, mine, c, record)
            b = words_at(mate_ref, m, mine, c, record)
            return jnp.where(mine == 0, a, b), jnp.where(mine == 0, b, a)

        scale = [scales(w) for w in words(width)]
        scale = [[s * norm[b : b + 1] for b, s in enumerate(pair)] for pair in scale]
        for c in range(width):
            for k, word in enumerate(words(c)):
                for b, q in enumerate(opened(word)):
                    row = (m * SUB * CORES + k) * width + c
                    flat[b, pl.ds(row, SUB, stride=CORES * width), :] = (q - MIDDLE) * scale[k][b]
    for b in range(2):
        out_ref[b] = (flat[b] * gain_ref[...]).astype(jnp.bfloat16)


def whole(space=pltpu.VMEM):
    return pl.BlockSpec(memory_space=space)


def room(mebibytes):
    return pltpu.CompilerParams(vmem_limit_bytes=mebibytes * 1024 * 1024)


def per_device(step_size, inputs, gate_input, decay_rate, norm_gain, resets):
    batch, width, _ = step_size.shape
    chips = lax.axis_size("seq_0") * lax.axis_size("seq_1")
    cores = lax.axis_size("seq_2")
    chan = lax.axis_size("chan")
    blocks = chips * cores
    record = width + 1
    rows = batch * width * blocks

    def as_rows(array):
        split = array.reshape(batch, width, blocks, LANES)
        return split.transpose(1, 2, 0, 3).reshape(rows, LANES)

    words = pl.pallas_call(
        functools.partial(scan_kernel, (batch, width, blocks, resets.shape[1])),
        out_shape=jax.ShapeDtypeStruct((blocks * record, LANES), jnp.int32),
        in_specs=[whole(pltpu.HBM)] * 5,
        out_specs=whole(),
        scratch_shapes=[
            pltpu.VMEM((3, rows, LANES), jnp.float32),
            pltpu.VMEM((batch * blocks, LANES), jnp.float32),
            pltpu.VMEM((batch * blocks, LANES), jnp.float32),
            pltpu.VMEM((2, 2 * SUB, LANES), jnp.float32),
            pltpu.VMEM((rows + batch * blocks, LANES), jnp.int32),
            *[pltpu.VMEM((rows, LANES), jnp.bfloat16)] * 3,
            pltpu.SMEM(decay_rate.shape, jnp.float32),
            pltpu.SMEM(resets.shape, jnp.int32),
            pltpu.SemaphoreType.DMA((3, width)),
            pltpu.SemaphoreType.DMA((2,)),
        ],
        compiler_params=room(16),
        name="scan",
    )(
        *[
            pltpu.with_memory_space_constraint(x, pltpu.HBM)
            for x in (decay_rate, resets, *map(as_rows, (step_size, inputs, gate_input)))
        ],
    )
    words = words.reshape(chips, cores * record, 1, LANES)
    words = lax.all_to_all(words, ("seq_0", "seq_1"), 0, 0, tiled=True)
    words = words.reshape(blocks * record, LANES)
    sums = pl.pallas_call(
        functools.partial(squares_kernel, (width, chips)),
        out_shape=jax.ShapeDtypeStruct((cores * chan, batch, LANES), jnp.float32),
        in_specs=[whole()],
        out_specs=whole(),
        compiler_params=room(8),
        name="squares",
    )(words)
    sums = lax.all_to_all(sums, ("seq_2", "chan"), 0, 0, tiled=True)
    mate = lax.ppermute(words, "seq_2", [(0, 1), (1, 0)])
    channels = blocks * width
    gain = pl.pallas_call(
        gain_kernel,
        out_shape=jax.ShapeDtypeStruct((channels, LANES), jnp.float32),
        in_specs=[whole()],
        out_specs=whole(),
        compiler_params=room(8),
        name="gain",
    )(norm_gain.reshape(channels // LANES, LANES))
    return pl.pallas_call(
        functools.partial(final_kernel, (width, chips)),
        out_shape=jax.ShapeDtypeStruct((batch, channels, LANES), jnp.bfloat16),
        in_specs=[whole()] * 4,
        out_specs=whole(),
        scratch_shapes=[pltpu.VMEM((batch, channels, LANES), jnp.float32)],
        compiler_params=room(8),
        name="final",
    )(words, mate, sums, gain)


def solution(mesh):
    split = Mesh(
        mesh.devices.reshape(8, 4, 2, mesh.shape["chan"]), ("seq_0", "seq_1", "seq_2", "chan")
    )
    in_specs = (
        P(None, CHAN_SEQ, None),
        P(None, CHAN_SEQ, None),
        P(None, CHAN_SEQ, None),
        P("chan"),
        P("chan"),
        P(),
    )
    out_specs = P(None, "chan", SEQ)

    return jax.shard_map(
        per_device, mesh=split, in_specs=in_specs, out_specs=out_specs, check_vma=False
    )
```

```python
import functools

import jax
import jax.numpy as jnp
from jax import lax
from jax.experimental import pallas as pl
from jax.experimental.pallas import tpu as pltpu
from jax.sharding import Mesh
from jax.sharding import PartitionSpec as P


FEATURE_WIDTH = 5120
SEQ = ("seq_0", "seq_1", "seq_2")
CHAN_SEQ = ("chan", "seq_0", "seq_1", "seq_2")
LANES = 128
SUB = 8
LEVELS = 32700.0
MIDDLE = 32768.0
FINE = 64.0
CODE_ZERO = 16384.0
CORES = 2
LOG2E = 1.4426950408889634
GROUP = 5


def root_of_one_minus_exp(x, expo):
    p = 1.0 / 6.0 - x * (1.0 / 24.0 - x * (1.0 / 120.0))
    p = x * (1.0 - x * (0.5 - x * p))
    y = jnp.where(x < 0.0625, p, 1.0 - expo * expo)
    return y * lax.rsqrt(jnp.maximum(y, 1e-37))


def tile(v):
    return slice(v * SUB, (v + 1) * SUB)


def scan_kernel(
    sizes,
    rate_hbm,
    reset_hbm,
    step_hbm,
    inp_hbm,
    gate_hbm,
    out_ref,
    held,
    live,
    top,
    tot,
    ints,
    step_ref,
    inp_ref,
    gate_ref,
    rate_ref,
    reset_ref,
    sems,
    small,
):
    batch, width, blocks, ndoc = sizes
    place = lax.axis_index(SEQ)
    count = batch * blocks
    tiles = LANES // SUB
    lane = lax.broadcasted_iota(jnp.int32, (SUB, LANES), 1)
    sub = lax.broadcasted_iota(jnp.int32, (SUB, LANES), 0)
    odd = (sub & 1) == 1

    sources = ((step_hbm, step_ref), (inp_hbm, inp_ref), (gate_hbm, gate_ref))

    def fetch(k, c):
        at = pl.ds(c * count, count)
        return pltpu.make_async_copy(sources[k][0].at[at], sources[k][1].at[at], sems.at[k, c])

    scalars = [
        pltpu.make_async_copy(rate_hbm, rate_ref, small.at[0]),
        pltpu.make_async_copy(reset_hbm, reset_ref, small.at[1]),
    ]
    for copy in scalars:
        copy.start()
    for c in range(width):
        fetch(0, c).start()
        fetch(1, c).start()
    for c in range(width):
        fetch(2, c).start()

    for copy in scalars:
        copy.wait()
    marks = [jnp.where(odd, reset_ref[1, k], reset_ref[0, k]) for k in range(ndoc)]
    for v in range(tiles):
        t = (v * (SUB // 2) + (sub >> 1)) * LANES + lane
        hit = t == marks[0]
        for mark in marks[1:]:
            hit = hit | (t == mark)
        live[tile(v), :] = jnp.where(hit, 0.0, 1.0)
        top[tile(v), :] = jnp.full((SUB, LANES), 1e-30, jnp.float32)
    tot[...] = jnp.zeros_like(tot)

    def local(c):
        at = tile_of(c, count)
        scaled = step_ref[at, :].astype(jnp.float32) * rate_ref[place * width + c]
        expo = jnp.exp2(scaled * (-LOG2E))
        drive = root_of_one_minus_exp(scaled + scaled, expo) * inp_ref[at, :].astype(jnp.float32)
        at_a = (expo * live[...]).T
        at_s = drive.T
        end_a = end_s = None
        for v in range(tiles):
            a, s = at_a[tile(v)], at_s[tile(v)]
            for k in (1, 2, 4):
                keep = sub >= k
                s = s + a * jnp.where(keep, pltpu.roll(s, k, 0), 0.0)
                a = a * jnp.where(keep, pltpu.roll(a, k, 0), 1.0)
            if v:
                s = s + a * end_s
                a = a * end_a
            here = tile(c * tiles + v)
            held[0, here, :] = a
            held[1, here, :] = s
            end_a = jnp.broadcast_to(a[SUB - 1 :], (SUB, LANES))
            end_s = jnp.broadcast_to(s[SUB - 1 :], (SUB, LANES))
        tot[0, c : c + 1, :] = end_a[:1]
        tot[1, c : c + 1, :] = end_s[:1]

    for low in range(0, width, GROUP):
        group = range(low, min(width, low + GROUP))
        for c in group:
            fetch(0, c).wait()
            fetch(1, c).wait()
        for c in group:
            local(c)
    for c in range(width):
        fetch(2, c).wait()

    wide = lax.broadcasted_iota(jnp.int32, tot.shape[1:], 1)
    a, s = tot[0], tot[1]
    span, offset = batch, batch
    while span < count:
        terms = []
        for k in range(4):
            shift = offset + k * span
            if shift >= count:
                break
            if not shift:
                terms.append((a, s))
                continue
            keep = wide >= shift
            terms.append(
                (
                    jnp.where(keep, pltpu.roll(a, shift, 1), 1.0),
                    jnp.where(keep, pltpu.roll(s, shift, 1), 0.0),
                )
            )
        a, s = terms[-1]
        for later_a, later_s in terms[-2::-1]:
            s = later_s + later_a * s
            a = later_a * a
        span, offset = span * 4, 0
    tot[0] = s

    def emit(c):
        at = tile_of(c, count)
        state = (held[1, at, :] + held[0, at, :] * tot[0, c : c + 1, :]).T
        g = gate_ref[at, :].astype(jnp.float32)
        value = state * (g / (1.0 + jnp.exp2(g * (-LOG2E))))
        held[2, at, :] = value
        top[...] = jnp.maximum(top[...], jnp.abs(value))

    for c in range(width):
        emit(c)

    e = jnp.ceil(jnp.log2(top[...]) * FINE)
    top[...] = jnp.exp2(e * (-1.0 / FINE)) * LEVELS
    ints[pl.ds(width * count, count), :] = (e + CODE_ZERO).astype(jnp.int32)
    for c in range(width):
        ints[tile_of(c, count), :] = (held[2, tile_of(c, count), :] * top[...] + (MIDDLE + 0.5)).astype(
            jnp.int32
        )
    record = width + 1
    for c in range(record):
        for m in range(blocks // SUB):
            base = c * count + m * SUB * batch
            first, second = [ints[pl.ds(base + b, SUB, stride=batch), :] for b in range(batch)]
            out_ref[pl.ds(m * SUB * record + c, SUB, stride=record), :] = first * 65536 | second


def tile_of(c, count):
    return slice(c * count, (c + 1) * count)


def opened(word):
    return (
        lax.shift_right_logical(word, 16).astype(jnp.float32),
        (word & 65535).astype(jnp.float32),
    )


def scales(word):
    return [jnp.exp2((e - CODE_ZERO) * (1.0 / FINE)) * (1.0 / LEVELS) for e in opened(word)]


def words_at(ref, m, k, c, record):
    return ref[pl.ds((m * SUB * CORES + k) * record + c, SUB, stride=CORES * record), :]


def squares_kernel(sizes, got_ref, sum_ref):
    width, chips = sizes
    record = width + 1
    chan = sum_ref.shape[0] // CORES
    for k in range(CORES):
        acc = [None, None]
        for m in range(chips // SUB):
            scale = scales(words_at(got_ref, m, k, width, record))
            part = [None, None]
            for c in range(width):
                for b, q in enumerate(opened(words_at(got_ref, m, k, c, record))):
                    v = q - MIDDLE
                    part[b] = v * v if part[b] is None else part[b] + v * v
            for b in range(2):
                more = part[b] * (scale[b] * scale[b])
                acc[b] = more if acc[b] is None else acc[b] + more
        for b in range(2):
            row = jnp.sum(acc[b], axis=0, keepdims=True)
            for y in range(chan):
                sum_ref[k * chan + y, b : b + 1, :] = row


def gain_kernel(gain_ref, out_ref):
    for g in range(out_ref.shape[0] // LANES):
        row = gain_ref[g : g + 1, :]
        out_ref[g * LANES : (g + 1) * LANES, :] = jnp.broadcast_to(row, (LANES, LANES)).T


def final_kernel(sizes, own_ref, mate_ref, sum_ref, gain_ref, out_ref, flat):
    width, chips = sizes
    mine = lax.axis_index("seq_2")
    record = width + 1
    total = sum_ref[0]
    for k in range(1, sum_ref.shape[0]):
        total = total + sum_ref[k]
    norm = lax.rsqrt(total / jnp.float32(FEATURE_WIDTH) + 1e-5)
    for m in range(chips // SUB):

        def words(c):
            a = words_at(own_ref, m, mine, c, record)
            b = words_at(mate_ref, m, mine, c, record)
            return jnp.where(mine == 0, a, b), jnp.where(mine == 0, b, a)

        scale = [scales(w) for w in words(width)]
        scale = [[s * norm[b : b + 1] for b, s in enumerate(pair)] for pair in scale]
        for c in range(width):
            for k, word in enumerate(words(c)):
                for b, q in enumerate(opened(word)):
                    row = (m * SUB * CORES + k) * width + c
                    flat[b, pl.ds(row, SUB, stride=CORES * width), :] = (q - MIDDLE) * scale[k][b]
    for b in range(2):
        out_ref[b] = (flat[b] * gain_ref[...]).astype(jnp.bfloat16)


def whole(space=pltpu.VMEM):
    return pl.BlockSpec(memory_space=space)


def room(mebibytes):
    return pltpu.CompilerParams(vmem_limit_bytes=mebibytes * 1024 * 1024)


def per_device(step_size, inputs, gate_input, decay_rate, norm_gain, resets):
    batch, width, _ = step_size.shape
    chips = lax.axis_size("seq_0") * lax.axis_size("seq_1")
    cores = lax.axis_size("seq_2")
    chan = lax.axis_size("chan")
    blocks = chips * cores
    record = width + 1
    rows = batch * width * blocks

    def as_rows(array):
        split = array.reshape(batch, width, blocks, LANES)
        return split.transpose(1, 2, 0, 3).reshape(rows, LANES)

    words = pl.pallas_call(
        functools.partial(scan_kernel, (batch, width, blocks, resets.shape[1])),
        out_shape=jax.ShapeDtypeStruct((blocks * record, LANES), jnp.int32),
        in_specs=[whole(pltpu.HBM)] * 5,
        out_specs=whole(),
        scratch_shapes=[
            pltpu.VMEM((3, rows, LANES), jnp.float32),
            pltpu.VMEM((batch * blocks, LANES), jnp.float32),
            pltpu.VMEM((batch * blocks, LANES), jnp.float32),
            pltpu.VMEM((2, 2 * SUB, LANES), jnp.float32),
            pltpu.VMEM((rows + batch * blocks, LANES), jnp.int32),
            *[pltpu.VMEM((rows, LANES), jnp.bfloat16)] * 3,
            pltpu.SMEM(decay_rate.shape, jnp.float32),
            pltpu.SMEM(resets.shape, jnp.int32),
            pltpu.SemaphoreType.DMA((3, width)),
            pltpu.SemaphoreType.DMA((2,)),
        ],
        compiler_params=room(16),
        name="scan",
    )(
        *[
            pltpu.with_memory_space_constraint(x, pltpu.HBM)
            for x in (decay_rate, resets, *map(as_rows, (step_size, inputs, gate_input)))
        ],
    )
    words = words.reshape(chips, cores * record, 1, LANES)
    words = lax.all_to_all(words, ("seq_0", "seq_1"), 0, 0, tiled=True)
    words = words.reshape(blocks * record, LANES)
    sums = pl.pallas_call(
        functools.partial(squares_kernel, (width, chips)),
        out_shape=jax.ShapeDtypeStruct((cores * chan, batch, LANES), jnp.float32),
        in_specs=[whole()],
        out_specs=whole(),
        compiler_params=room(8),
        name="squares",
    )(words)
    sums = lax.all_to_all(sums, ("seq_2", "chan"), 0, 0, tiled=True)
    mate = lax.ppermute(words, "seq_2", [(0, 1), (1, 0)])
    channels = blocks * width
    gain = pl.pallas_call(
        gain_kernel,
        out_shape=jax.ShapeDtypeStruct((channels, LANES), jnp.float32),
        in_specs=[whole()],
        out_specs=whole(),
        compiler_params=room(8),
        name="gain",
    )(norm_gain.reshape(channels // LANES, LANES))
    return pl.pallas_call(
        functools.partial(final_kernel, (width, chips)),
        out_shape=jax.ShapeDtypeStruct((batch, channels, LANES), jnp.bfloat16),
        in_specs=[whole()] * 4,
        out_specs=whole(),
        scratch_shapes=[pltpu.VMEM((batch, channels, LANES), jnp.float32)],
        compiler_params=room(8),
        name="final",
    )(words, mate, sums, gain)


def solution(mesh):
    split = Mesh(
        mesh.devices.reshape(8, 4, 2, mesh.shape["chan"]), ("seq_0", "seq_1", "seq_2", "chan")
    )
    in_specs = (
        P(None, CHAN_SEQ, None),
        P(None, CHAN_SEQ, None),
        P(None, CHAN_SEQ, None),
        P("chan"),
        P("chan"),
        P(),
    )
    out_specs = P(None, "chan", SEQ)

    return jax.shard_map(
        per_device, mesh=split, in_specs=in_specs, out_specs=out_specs, check_vma=False
    )
```

```python
import functools

import jax
import jax.numpy as jnp
from jax import lax
from jax.experimental import pallas as pl
from jax.experimental.pallas import tpu as pltpu
from jax.sharding import Mesh
from jax.sharding import PartitionSpec as P


FEATURE_WIDTH = 5120
SEQ = ("seq_0", "seq_1", "seq_2")
CHAN_SEQ = ("chan", "seq_0", "seq_1", "seq_2")
LANES = 128
SUB = 8
LEVELS = 32700.0
MIDDLE = 32768.0
FINE = 64.0
CODE_ZERO = 16384.0
CORES = 2
LOG2E = 1.4426950408889634
GROUP = 5
TURN = 6
SIDE = 2
HEAD_CORE = 1
HEAD_CHAN = 5


def root_of_one_minus_exp(x, expo):
    p = 1.0 / 6.0 - x * (1.0 / 24.0 - x * (1.0 / 120.0))
    p = x * (1.0 - x * (0.5 - x * p))
    y = jnp.where(x < 0.0625, p, 1.0 - expo * expo)
    return y * lax.rsqrt(jnp.maximum(y, 1e-37))


def tile(v):
    return slice(v * SUB, (v + 1) * SUB)


def scan_kernel(
    sizes,
    rate_hbm,
    reset_hbm,
    step_hbm,
    inp_hbm,
    gate_hbm,
    out_ref,
    held,
    live,
    top,
    tot,
    ints,
    step_ref,
    inp_ref,
    gate_ref,
    rate_ref,
    reset_ref,
    sems,
    small,
):
    batch, width, blocks, ndoc = sizes
    place = lax.axis_index(SEQ)
    count = batch * blocks
    tiles = LANES // SUB
    lane = lax.broadcasted_iota(jnp.int32, (SUB, LANES), 1)
    sub = lax.broadcasted_iota(jnp.int32, (SUB, LANES), 0)
    odd = (sub & 1) == 1

    sources = ((step_hbm, step_ref), (inp_hbm, inp_ref), (gate_hbm, gate_ref))

    def fetch(k, c):
        at = pl.ds(c * count, count)
        return pltpu.make_async_copy(sources[k][0].at[at], sources[k][1].at[at], sems.at[k, c])

    scalars = [
        pltpu.make_async_copy(rate_hbm, rate_ref, small.at[0]),
        pltpu.make_async_copy(reset_hbm, reset_ref, small.at[1]),
    ]
    for copy in scalars:
        copy.start()
    for c in range(width):
        fetch(0, c).start()
        fetch(1, c).start()
    for c in range(width):
        fetch(2, c).start()

    for copy in scalars:
        copy.wait()
    marks = [jnp.where(odd, reset_ref[1, k], reset_ref[0, k]) for k in range(ndoc)]
    for v in range(tiles):
        t = (v * (SUB // 2) + (sub >> 1)) * LANES + lane
        hit = t == marks[0]
        for mark in marks[1:]:
            hit = hit | (t == mark)
        live[tile(v), :] = jnp.where(hit, 0.0, 1.0)
        top[tile(v), :] = jnp.full((SUB, LANES), 1e-30, jnp.float32)
    tot[...] = jnp.zeros_like(tot)

    def local(c):
        at = tile_of(c, count)
        scaled = step_ref[at, :].astype(jnp.float32) * rate_ref[place * width + c]
        expo = jnp.exp2(scaled * (-LOG2E))
        drive = root_of_one_minus_exp(scaled + scaled, expo) * inp_ref[at, :].astype(jnp.float32)
        at_a = (expo * live[...]).T
        at_s = drive.T
        end_a = end_s = None
        for v in range(tiles):
            a, s = at_a[tile(v)], at_s[tile(v)]
            for k in (1, 2, 4):
                keep = sub >= k
                s = s + a * jnp.where(keep, pltpu.roll(s, k, 0), 0.0)
                a = a * jnp.where(keep, pltpu.roll(a, k, 0), 1.0)
            if v:
                s = s + a * end_s
                a = a * end_a
            here = tile(c * tiles + v)
            held[0, here, :] = a
            held[1, here, :] = s
            end_a = jnp.broadcast_to(a[SUB - 1 :], (SUB, LANES))
            end_s = jnp.broadcast_to(s[SUB - 1 :], (SUB, LANES))
        tot[0, c : c + 1, :] = end_a[:1]
        tot[1, c : c + 1, :] = end_s[:1]

    for low in range(0, width, GROUP):
        group = range(low, min(width, low + GROUP))
        for c in group:
            fetch(0, c).wait()
            fetch(1, c).wait()
        for c in group:
            local(c)
    for c in range(width):
        fetch(2, c).wait()

    wide = lax.broadcasted_iota(jnp.int32, tot.shape[1:], 1)
    a, s = tot[0], tot[1]
    span, offset = batch, batch
    while span < count:
        terms = []
        for k in range(4):
            shift = offset + k * span
            if shift >= count:
                break
            if not shift:
                terms.append((a, s))
                continue
            keep = wide >= shift
            terms.append(
                (
                    jnp.where(keep, pltpu.roll(a, shift, 1), 1.0),
                    jnp.where(keep, pltpu.roll(s, shift, 1), 0.0),
                )
            )
        a, s = terms[-1]
        for later_a, later_s in terms[-2::-1]:
            s = later_s + later_a * s
            a = later_a * a
        span, offset = span * 4, 0
    tot[0] = s

    def emit(c):
        at = tile_of(c, count)
        state = (held[1, at, :] + held[0, at, :] * tot[0, c : c + 1, :]).T
        g = gate_ref[at, :].astype(jnp.float32)
        value = state * (g / (1.0 + jnp.exp2(g * (-LOG2E))))
        held[2, at, :] = value
        top[...] = jnp.maximum(top[...], jnp.abs(value))

    for c in range(width):
        emit(c)

    e = jnp.ceil(jnp.log2(top[...]) * FINE)
    top[...] = jnp.exp2(e * (-1.0 / FINE)) * LEVELS
    ints[pl.ds(width * count, count), :] = (e + CODE_ZERO).astype(jnp.int32)
    for c in range(width):
        ints[tile_of(c, count), :] = (held[2, tile_of(c, count), :] * top[...] + (MIDDLE + 0.5)).astype(
            jnp.int32
        )
    record = width + 1
    for c in range(record):
        for m in range(blocks // SUB):
            base = c * count + m * SUB * batch
            first, second = [ints[pl.ds(base + b, SUB, stride=batch), :] for b in range(batch)]
            to = (m - TURN) % (blocks // SUB) * SUB * record + c
            word = pltpu.roll(first * 65536 | second, SUB - SIDE * CORES, 0)
            out_ref[pl.ds(to, SUB, stride=record), :] = word


def tile_of(c, count):
    return slice(c * count, (c + 1) * count)


def opened(word):
    return (
        lax.shift_right_logical(word, 16).astype(jnp.float32),
        (word & 65535).astype(jnp.float32),
    )


def scales(word):
    return [jnp.exp2((e - CODE_ZERO) * (1.0 / FINE)) * (1.0 / LEVELS) for e in opened(word)]


def words_at(ref, m, k, c, record):
    return ref[pl.ds((m * SUB * CORES + k) * record + c, SUB, stride=CORES * record), :]


def squares_kernel(sizes, got_ref, sum_ref):
    width, chips = sizes
    record = width + 1
    chan = sum_ref.shape[0] // CORES
    for k in range(CORES):
        acc = [None, None]
        for m in range(chips // SUB):
            scale = scales(words_at(got_ref, m, k, width, record))
            part = [None, None]
            for c in range(width):
                for b, q in enumerate(opened(words_at(got_ref, m, k, c, record))):
                    v = q - MIDDLE
                    part[b] = v * v if part[b] is None else part[b] + v * v
            for b in range(2):
                more = part[b] * (scale[b] * scale[b])
                acc[b] = more if acc[b] is None else acc[b] + more
        for b in range(2):
            row = jnp.sum(acc[b], axis=0, keepdims=True)
            for y in range(chan):
                sum_ref[(k - HEAD_CORE) % CORES * chan + y, b : b + 1, :] = row


def straight(word):
    sub = lax.broadcasted_iota(jnp.int32, (SUB, LANES), 0)
    return jnp.where((sub & 2) == 0, pltpu.roll(word, SUB - SIDE, 0), pltpu.roll(word, SIDE, 0))


def gain_kernel(gain_ref, out_ref):
    for g in range(out_ref.shape[0] // LANES):
        row = gain_ref[g : g + 1, :]
        out_ref[g * LANES : (g + 1) * LANES, :] = jnp.broadcast_to(row, (LANES, LANES)).T


def final_kernel(sizes, own_ref, mate_ref, sum_ref, gain_ref, out_ref, flat):
    width, chips = sizes
    mine = lax.axis_index("seq_2")
    record = width + 1
    total = sum_ref[0]
    for k in range(1, sum_ref.shape[0]):
        total = total + sum_ref[k]
    norm = lax.rsqrt(total / jnp.float32(FEATURE_WIDTH) + 1e-5)
    for m in range(chips // SUB):

        def words(c):
            a = words_at(own_ref, m, mine, c, record)
            b = words_at(mate_ref, m, mine, c, record)
            return straight(jnp.where(mine == 0, a, b)), straight(jnp.where(mine == 0, b, a))

        scale = [scales(w) for w in words(width)]
        scale = [[s * norm[b : b + 1] for b, s in enumerate(pair)] for pair in scale]
        for c in range(width):
            for k, word in enumerate(words(c)):
                for b, q in enumerate(opened(word)):
                    row = ((m + TURN // 2) % (chips // SUB) * SUB * CORES + k) * width + c
                    flat[b, pl.ds(row, SUB, stride=CORES * width), :] = (q - MIDDLE) * scale[k][b]
    for b in range(2):
        out_ref[b] = (flat[b] * gain_ref[...]).astype(jnp.bfloat16)


def whole(space=pltpu.VMEM):
    return pl.BlockSpec(memory_space=space)


def room(mebibytes):
    return pltpu.CompilerParams(vmem_limit_bytes=mebibytes * 1024 * 1024)


def per_device(step_size, inputs, gate_input, decay_rate, norm_gain, resets):
    batch, width, _ = step_size.shape
    chips = lax.axis_size("seq_0") * lax.axis_size("seq_1")
    cores = lax.axis_size("seq_2")
    chan = lax.axis_size("chan")
    blocks = chips * cores
    record = width + 1
    rows = batch * width * blocks

    def as_rows(array):
        split = array.reshape(batch, width, blocks, LANES)
        return split.transpose(1, 2, 0, 3).reshape(rows, LANES)

    words = pl.pallas_call(
        functools.partial(scan_kernel, (batch, width, blocks, resets.shape[1])),
        out_shape=jax.ShapeDtypeStruct((blocks * record, LANES), jnp.int32),
        in_specs=[whole(pltpu.HBM)] * 5,
        out_specs=whole(),
        scratch_shapes=[
            pltpu.VMEM((3, rows, LANES), jnp.float32),
            pltpu.VMEM((batch * blocks, LANES), jnp.float32),
            pltpu.VMEM((batch * blocks, LANES), jnp.float32),
            pltpu.VMEM((2, 2 * SUB, LANES), jnp.float32),
            pltpu.VMEM((rows + batch * blocks, LANES), jnp.int32),
            *[pltpu.VMEM((rows, LANES), jnp.bfloat16)] * 3,
            pltpu.SMEM(decay_rate.shape, jnp.float32),
            pltpu.SMEM(resets.shape, jnp.int32),
            pltpu.SemaphoreType.DMA((3, width)),
            pltpu.SemaphoreType.DMA((2,)),
        ],
        compiler_params=room(16),
        name="scan",
    )(
        *[
            pltpu.with_memory_space_constraint(x, pltpu.HBM)
            for x in (decay_rate, resets, *map(as_rows, (step_size, inputs, gate_input)))
        ],
    )
    words = words.reshape(chips, cores * record, 1, LANES)
    deep, side = lax.axis_size("seq_0"), lax.axis_size("seq_1")
    turned = [
        [(z + TURN) % deep * side + (x + SIDE) % side for z in range(deep) for x in range(side)]
    ]
    words = lax.all_to_all(
        words, ("seq_0", "seq_1"), 0, 0, axis_index_groups=turned, tiled=True
    )
    words = words.reshape(blocks * record, LANES)
    sums = pl.pallas_call(
        functools.partial(squares_kernel, (width, chips)),
        out_shape=jax.ShapeDtypeStruct((cores * chan, batch, LANES), jnp.float32),
        in_specs=[whole()],
        out_specs=whole(),
        compiler_params=room(8),
        name="squares",
    )(words)
    order = [
        [
            (k + HEAD_CORE) % cores * chan + (y + HEAD_CHAN) % chan
            for k in range(cores)
            for y in range(chan)
        ]
    ]
    sums = lax.all_to_all(
        sums, ("seq_2", "chan"), 0, 0, axis_index_groups=order, tiled=True
    )
    mate = lax.ppermute(words, "seq_2", [(0, 1), (1, 0)])
    channels = blocks * width
    gain = pl.pallas_call(
        gain_kernel,
        out_shape=jax.ShapeDtypeStruct((channels, LANES), jnp.float32),
        in_specs=[whole()],
        out_specs=whole(),
        compiler_params=room(8),
        name="gain",
    )(norm_gain.reshape(channels // LANES, LANES))
    return pl.pallas_call(
        functools.partial(final_kernel, (width, chips)),
        out_shape=jax.ShapeDtypeStruct((batch, channels, LANES), jnp.bfloat16),
        in_specs=[whole()] * 4,
        out_specs=whole(),
        scratch_shapes=[pltpu.VMEM((batch, channels, LANES), jnp.float32)],
        compiler_params=room(8),
        name="final",
    )(words, mate, sums, gain)


def solution(mesh):
    split = Mesh(
        mesh.devices.reshape(8, 4, 2, mesh.shape["chan"]), ("seq_0", "seq_1", "seq_2", "chan")
    )
    in_specs = (
        P(None, CHAN_SEQ, None),
        P(None, CHAN_SEQ, None),
        P(None, CHAN_SEQ, None),
        P("chan"),
        P("chan"),
        P(),
    )
    out_specs = P(None, "chan", SEQ)

    return jax.shard_map(
        per_device, mesh=split, in_specs=in_specs, out_specs=out_specs, check_vma=False
    )
```

```python
import functools

import jax
import jax.numpy as jnp
from jax import lax
from jax.experimental import pallas as pl
from jax.experimental.pallas import tpu as pltpu
from jax.sharding import Mesh
from jax.sharding import PartitionSpec as P


FEATURE_WIDTH = 5120
SEQ = ("seq_0", "seq_1", "seq_2")
CHAN_SEQ = ("chan", "seq_0", "seq_1", "seq_2")
LANES = 128
SUB = 8
LEVELS = 32700.0
MIDDLE = 32768.0
FINE = 64.0
CODE_ZERO = 16384.0
CORES = 2
LOG2E = 1.4426950408889634
EDGES = (0, 2, 10)
TURN = 6
SIDE = 2
HEAD_CORE = 1
HEAD_CHAN = 5


def root_of_one_minus_exp(x, expo):
    p = 1.0 / 6.0 - x * (1.0 / 24.0 - x * (1.0 / 120.0))
    p = x * (1.0 - x * (0.5 - x * p))
    y = jnp.where(x < 0.0625, p, 1.0 - expo * expo)
    return y * lax.rsqrt(jnp.maximum(y, 1e-37))


def tile(v):
    return slice(v * SUB, (v + 1) * SUB)


def scan_kernel(
    sizes,
    rate_hbm,
    reset_hbm,
    step_hbm,
    inp_hbm,
    gate_hbm,
    out_ref,
    held,
    live,
    top,
    tot,
    ints,
    step_ref,
    inp_ref,
    gate_ref,
    rate_ref,
    reset_ref,
    sems,
    small,
):
    batch, width, blocks, ndoc = sizes
    place = lax.axis_index(SEQ)
    count = batch * blocks
    tiles = LANES // SUB
    lane = lax.broadcasted_iota(jnp.int32, (SUB, LANES), 1)
    sub = lax.broadcasted_iota(jnp.int32, (SUB, LANES), 0)
    odd = (sub & 1) == 1

    sources = ((step_hbm, step_ref), (inp_hbm, inp_ref), (gate_hbm, gate_ref))

    def fetch(k, c):
        at = pl.ds(c * count, count)
        return pltpu.make_async_copy(sources[k][0].at[at], sources[k][1].at[at], sems.at[k, c])

    scalars = [
        pltpu.make_async_copy(rate_hbm, rate_ref, small.at[0]),
        pltpu.make_async_copy(reset_hbm, reset_ref, small.at[1]),
    ]
    for copy in scalars:
        copy.start()
    for c in range(width):
        fetch(0, c).start()
        fetch(1, c).start()
    for c in range(width):
        fetch(2, c).start()

    for copy in scalars:
        copy.wait()
    marks = [jnp.where(odd, reset_ref[1, k], reset_ref[0, k]) for k in range(ndoc)]
    for v in range(tiles):
        t = (v * (SUB // 2) + (sub >> 1)) * LANES + lane
        hit = t == marks[0]
        for mark in marks[1:]:
            hit = hit | (t == mark)
        live[tile(v), :] = jnp.where(hit, 0.0, 1.0)
        top[tile(v), :] = jnp.full((SUB, LANES), 1e-30, jnp.float32)
    tot[...] = jnp.zeros_like(tot)

    def local(c):
        at = tile_of(c, count)
        scaled = step_ref[at, :].astype(jnp.float32) * rate_ref[place * width + c]
        expo = jnp.exp2(scaled * (-LOG2E))
        drive = root_of_one_minus_exp(scaled + scaled, expo) * inp_ref[at, :].astype(jnp.float32)
        at_a = (expo * live[...]).T
        at_s = drive.T
        end_a = end_s = None
        for v in range(tiles):
            a, s = at_a[tile(v)], at_s[tile(v)]
            for k in (1, 2, 4):
                keep = sub >= k
                s = s + a * jnp.where(keep, pltpu.roll(s, k, 0), 0.0)
                a = a * jnp.where(keep, pltpu.roll(a, k, 0), 1.0)
            if v:
                s = s + a * end_s
                a = a * end_a
            here = tile(c * tiles + v)
            held[0, here, :] = a
            held[1, here, :] = s
            end_a = jnp.broadcast_to(a[SUB - 1 :], (SUB, LANES))
            end_s = jnp.broadcast_to(s[SUB - 1 :], (SUB, LANES))
        tot[0, c : c + 1, :] = end_a[:1]
        tot[1, c : c + 1, :] = end_s[:1]

    for low, high in zip(EDGES, (*EDGES[1:], width)):
        group = range(min(low, width), min(high, width))
        for c in group:
            fetch(0, c).wait()
            fetch(1, c).wait()
        for c in group:
            local(c)
    for c in range(width):
        fetch(2, c).wait()

    wide = lax.broadcasted_iota(jnp.int32, tot.shape[1:], 1)
    a, s = tot[0], tot[1]
    span, offset = batch, batch
    while span < count:
        terms = []
        for k in range(4):
            shift = offset + k * span
            if shift >= count:
                break
            if not shift:
                terms.append((a, s))
                continue
            keep = wide >= shift
            terms.append(
                (
                    jnp.where(keep, pltpu.roll(a, shift, 1), 1.0),
                    jnp.where(keep, pltpu.roll(s, shift, 1), 0.0),
                )
            )
        a, s = terms[-1]
        for later_a, later_s in terms[-2::-1]:
            s = later_s + later_a * s
            a = later_a * a
        span, offset = span * 4, 0
    tot[0] = s

    def emit(c):
        at = tile_of(c, count)
        state = (held[1, at, :] + held[0, at, :] * tot[0, c : c + 1, :]).T
        g = gate_ref[at, :].astype(jnp.float32)
        value = state * (g / (1.0 + jnp.exp2(g * (-LOG2E))))
        held[2, at, :] = value
        top[...] = jnp.maximum(top[...], jnp.abs(value))

    for c in range(width):
        emit(c)

    e = jnp.ceil(jnp.log2(top[...]) * FINE)
    top[...] = jnp.exp2(e * (-1.0 / FINE)) * LEVELS
    ints[pl.ds(width * count, count), :] = (e + CODE_ZERO).astype(jnp.int32)
    for c in range(width):
        ints[tile_of(c, count), :] = (held[2, tile_of(c, count), :] * top[...] + (MIDDLE + 0.5)).astype(
            jnp.int32
        )
    record = width + 1
    for c in range(record):
        for m in range(blocks // SUB):
            base = c * count + m * SUB * batch
            first, second = [ints[pl.ds(base + b, SUB, stride=batch), :] for b in range(batch)]
            to = (m - TURN) % (blocks // SUB) * SUB * record + c
            word = pltpu.roll(first * 65536 | second, SUB - SIDE * CORES, 0)
            out_ref[pl.ds(to, SUB, stride=record), :] = word


def tile_of(c, count):
    return slice(c * count, (c + 1) * count)


def opened(word):
    return (
        lax.shift_right_logical(word, 16).astype(jnp.float32),
        (word & 65535).astype(jnp.float32),
    )


def scales(word):
    return [jnp.exp2((e - CODE_ZERO) * (1.0 / FINE)) * (1.0 / LEVELS) for e in opened(word)]


def words_at(ref, m, k, c, record):
    return ref[pl.ds((m * SUB * CORES + k) * record + c, SUB, stride=CORES * record), :]


def squares_kernel(sizes, got_ref, sum_ref):
    width, chips = sizes
    record = width + 1
    chan = sum_ref.shape[0] // CORES
    for k in range(CORES):
        acc = [None, None]
        for m in range(chips // SUB):
            scale = scales(words_at(got_ref, m, k, width, record))
            part = [None, None]
            for c in range(width):
                for b, q in enumerate(opened(words_at(got_ref, m, k, c, record))):
                    v = q - MIDDLE
                    part[b] = v * v if part[b] is None else part[b] + v * v
            for b in range(2):
                more = part[b] * (scale[b] * scale[b])
                acc[b] = more if acc[b] is None else acc[b] + more
        for b in range(2):
            row = jnp.sum(acc[b], axis=0, keepdims=True)
            for y in range(chan):
                sum_ref[(k - HEAD_CORE) % CORES * chan + y, b : b + 1, :] = row


def straight(word):
    sub = lax.broadcasted_iota(jnp.int32, (SUB, LANES), 0)
    return jnp.where((sub & 2) == 0, pltpu.roll(word, SUB - SIDE, 0), pltpu.roll(word, SIDE, 0))


def gain_kernel(gain_ref, out_ref):
    for g in range(out_ref.shape[0] // LANES):
        row = gain_ref[g : g + 1, :]
        out_ref[g * LANES : (g + 1) * LANES, :] = jnp.broadcast_to(row, (LANES, LANES)).T


def final_kernel(sizes, own_ref, mate_ref, sum_ref, gain_ref, out_hbm, flat, out_ref, sems):
    width, chips = sizes
    mine = lax.axis_index("seq_2")
    record = width + 1
    total = sum_ref[0]
    for k in range(1, sum_ref.shape[0]):
        total = total + sum_ref[k]
    norm = lax.rsqrt(total / jnp.float32(FEATURE_WIDTH) + 1e-5)
    for m in range(chips // SUB):

        def words(c):
            a = words_at(own_ref, m, mine, c, record)
            b = words_at(mate_ref, m, mine, c, record)
            return straight(jnp.where(mine == 0, a, b)), straight(jnp.where(mine == 0, b, a))

        scale = [scales(w) for w in words(width)]
        scale = [[s * norm[b : b + 1] for b, s in enumerate(pair)] for pair in scale]
        for c in range(width):
            for k, word in enumerate(words(c)):
                for b, q in enumerate(opened(word)):
                    row = ((m + TURN // 2) % (chips // SUB) * SUB * CORES + k) * width + c
                    flat[b, pl.ds(row, SUB, stride=CORES * width), :] = (q - MIDDLE) * scale[k][b]
    copies = []
    for b in range(2):
        out_ref[b] = (flat[b] * gain_ref[...]).astype(jnp.bfloat16)
        copies.append(pltpu.make_async_copy(out_ref.at[b], out_hbm.at[b], sems.at[b]))
        copies[-1].start()
    for copy in copies:
        copy.wait()


def whole(space=pltpu.VMEM):
    return pl.BlockSpec(memory_space=space)


def room(mebibytes):
    return pltpu.CompilerParams(vmem_limit_bytes=mebibytes * 1024 * 1024)


def per_device(step_size, inputs, gate_input, decay_rate, norm_gain, resets):
    batch, width, _ = step_size.shape
    chips = lax.axis_size("seq_0") * lax.axis_size("seq_1")
    cores = lax.axis_size("seq_2")
    chan = lax.axis_size("chan")
    blocks = chips * cores
    record = width + 1
    rows = batch * width * blocks

    def as_rows(array):
        split = array.reshape(batch, width, blocks, LANES)
        return split.transpose(1, 2, 0, 3).reshape(rows, LANES)

    words = pl.pallas_call(
        functools.partial(scan_kernel, (batch, width, blocks, resets.shape[1])),
        out_shape=jax.ShapeDtypeStruct((blocks * record, LANES), jnp.int32),
        in_specs=[whole(pltpu.HBM)] * 5,
        out_specs=whole(),
        scratch_shapes=[
            pltpu.VMEM((3, rows, LANES), jnp.float32),
            pltpu.VMEM((batch * blocks, LANES), jnp.float32),
            pltpu.VMEM((batch * blocks, LANES), jnp.float32),
            pltpu.VMEM((2, 2 * SUB, LANES), jnp.float32),
            pltpu.VMEM((rows + batch * blocks, LANES), jnp.int32),
            *[pltpu.VMEM((rows, LANES), jnp.bfloat16)] * 3,
            pltpu.SMEM(decay_rate.shape, jnp.float32),
            pltpu.SMEM(resets.shape, jnp.int32),
            pltpu.SemaphoreType.DMA((3, width)),
            pltpu.SemaphoreType.DMA((2,)),
        ],
        compiler_params=room(16),
        name="scan",
    )(
        *[
            pltpu.with_memory_space_constraint(x, pltpu.HBM)
            for x in (decay_rate, resets, *map(as_rows, (step_size, inputs, gate_input)))
        ],
    )
    words = words.reshape(chips, cores * record, 1, LANES)
    deep, side = lax.axis_size("seq_0"), lax.axis_size("seq_1")
    turned = [
        [(z + TURN) % deep * side + (x + SIDE) % side for z in range(deep) for x in range(side)]
    ]
    words = lax.all_to_all(
        words, ("seq_0", "seq_1"), 0, 0, axis_index_groups=turned, tiled=True
    )
    words = words.reshape(blocks * record, LANES)
    sums = pl.pallas_call(
        functools.partial(squares_kernel, (width, chips)),
        out_shape=jax.ShapeDtypeStruct((cores * chan, batch, LANES), jnp.float32),
        in_specs=[whole()],
        out_specs=whole(),
        compiler_params=room(8),
        name="squares",
    )(words)
    order = [
        [
            (k + HEAD_CORE) % cores * chan + (y + HEAD_CHAN) % chan
            for k in range(cores)
            for y in range(chan)
        ]
    ]
    sums = lax.all_to_all(
        sums, ("seq_2", "chan"), 0, 0, axis_index_groups=order, tiled=True
    )
    mate = lax.ppermute(words, "seq_2", [(0, 1), (1, 0)])
    channels = blocks * width
    gain = pl.pallas_call(
        gain_kernel,
        out_shape=jax.ShapeDtypeStruct((channels, LANES), jnp.float32),
        in_specs=[whole()],
        out_specs=whole(),
        compiler_params=room(8),
        name="gain",
    )(norm_gain.reshape(channels // LANES, LANES))
    return pl.pallas_call(
        functools.partial(final_kernel, (width, chips)),
        out_shape=jax.ShapeDtypeStruct((batch, channels, LANES), jnp.bfloat16),
        in_specs=[whole()] * 4,
        out_specs=whole(pltpu.HBM),
        scratch_shapes=[
            pltpu.VMEM((batch, channels, LANES), jnp.float32),
            pltpu.VMEM((batch, channels, LANES), jnp.bfloat16),
            pltpu.SemaphoreType.DMA((2,)),
        ],
        compiler_params=room(8),
        name="final",
    )(words, mate, sums, gain)


def solution(mesh):
    split = Mesh(
        mesh.devices.reshape(8, 4, 2, mesh.shape["chan"]), ("seq_0", "seq_1", "seq_2", "chan")
    )
    in_specs = (
        P(None, CHAN_SEQ, None),
        P(None, CHAN_SEQ, None),
        P(None, CHAN_SEQ, None),
        P("chan"),
        P("chan"),
        P(),
    )
    out_specs = P(None, "chan", SEQ)

    return jax.shard_map(
        per_device, mesh=split, in_specs=in_specs, out_specs=out_specs, check_vma=False
    )
```
